256 devices in a mesh: heads: 8 (over y, core), tok: 32 (over x, z).
Axes of the slice: x: 4, y: 4, z: 8, core: 2. Of those that a mesh axis runs over, the one named last changes fastest.
Arguments:
- video_q: bfloat16 [32768, 2048], P('tok', 'heads'), as said below
- video_k: bfloat16 [32768, 2048], P('tok', 'heads'), as said below
- video_v: bfloat16 [32768, 2048], P('tok', 'heads'), may hold values from -6 to 6
- audio_q: bfloat16 [2048, 2048], P('tok', 'heads'), as said below
- audio_k: bfloat16 [2048, 2048], P('tok', 'heads'), as said below
- audio_v: bfloat16 [2048, 2048], P('tok', 'heads'), may hold values from -6 to 6
- video_q_gain: float32 [2048], P('heads'), may hold values from 0.1 to 1.9
- audio_k_gain: float32 [2048], P('heads'), may hold values from 0.1 to 1.9
- audio_q_gain: float32 [2048], P('heads'), may hold values from 0.1 to 1.9
- video_k_gain: float32 [2048], P('heads'), may hold values from 0.1 to 1.9
Outputs:
- video_out: bfloat16 [32768, 2048], P('tok', 'heads')
- audio_out: bfloat16 [2048, 2048], P('tok', 'heads')
The draws below stay inside these ranges and needn't reach their ends.
Inputs may be any that keep to these rules, and one draw needn't show every extreme that they name: `video_q`: no row is zero. `video_k`: no row is zero. `audio_q`: no row is zero. `audio_k`: no row is zero.
All inputs are finite; a program needn't handle non-finite values.
Results may differ from the reference program's by a relative error of at most 0.012.
The reference program's roundings to bfloat16 on the way count: a program that leaves them out, or rounds other values in their place, can miss the bound.
Values may be sent and summed in bfloat16 or wider, within the bound.
A program may use at most 64 MiB of HBM per device.

```python
import math
import jax
import jax.numpy as jnp
from jax import lax

HEADS = 32
HD = 64
TOK_V = 1024
WIDTH = 2048
TOKENS = 32768
AUDIO = 2048
N_TOK = 32


def texture(key, count):
    first_key, second_key, third_key = jax.random.split(key, 3)
    base = jax.random.normal(first_key, (count, WIDTH), jnp.float32)
    column = jnp.exp(jnp.log(3.0) * jnp.arange(WIDTH, dtype=jnp.float32) / (WIDTH - 1))
    column = column * jnp.exp(jax.random.uniform(second_key, (WIDTH,), jnp.float32) * jnp.log(2.5))
    row_scale = jnp.exp(jax.random.uniform(third_key, (count, 1), jnp.float32) * jnp.log(10.0))
    return base * column * row_scale


def beacons(key):
    shared = jax.random.fold_in(key, 4242)
    first_key, second_key, third_key = jax.random.split(shared, 3)
    index = jnp.arange(4)
    owner = index * HEADS // 4
    heads_of = jnp.arange(WIDTH) // HD
    inside = (heads_of[None, :] == owner[:, None]).astype(jnp.float32)
    strength = 0.03 * (index.astype(jnp.float32)[:, None] + 1.0)
    direction = jax.random.normal(first_key, (4, WIDTH), jnp.float32)
    background = jax.random.normal(second_key, (4, WIDTH), jnp.float32) * strength
    vectors = inside * direction + (1.0 - inside) * background
    nudge = (1.0 - inside) * 0.02 * jax.random.normal(third_key, (4, WIDTH), jnp.float32)
    return (vectors, vectors + nudge)


def draw_video_q(key, part):
    values = texture(jax.random.fold_in(key, 11), TOKENS)
    vectors, nudged = beacons(key)
    values = values.at[jnp.arange(4) * (TOKENS // 4) + 5].set(vectors)
    return values.astype(jnp.bfloat16)


def draw_audio_k(key, part):
    values = texture(jax.random.fold_in(key, 12), AUDIO)
    vectors, nudged = beacons(key)
    values = values.at[jnp.arange(4) * (AUDIO // 4) + 1].set(vectors)
    values = values.at[jnp.arange(4) * (AUDIO // 4) + 2].set(nudged)
    return values.astype(jnp.bfloat16)


def draw_audio_q(key, part):
    values = texture(jax.random.fold_in(key, 13), AUDIO)
    vectors, nudged = beacons(key)
    values = values.at[jnp.arange(4) * (AUDIO // 4) + 3].set(vectors)
    return values.astype(jnp.bfloat16)


def draw_video_k(key, part):
    values = texture(jax.random.fold_in(key, 14), TOKENS)
    vectors, nudged = beacons(key)
    values = values.at[jnp.arange(4) * (TOKENS // 4) + 7].set(vectors)
    values = values.at[jnp.arange(4) * (TOKENS // 4) + 8].set(nudged)
    return values.astype(jnp.bfloat16)


def level_of(stream_key, extent, shards, least, high):
    level = 1.0
    for axis_at, blocks in shards:
        steps = jax.random.uniform(jax.random.fold_in(jax.random.fold_in(stream_key, 6), axis_at), (blocks,), jnp.float32, least / len(shards), high / len(shards))
        level = level * jnp.repeat(jnp.exp(steps), extent[axis_at] // blocks).reshape((-1,) + (1,) * (len(extent) - 1 - axis_at))
    return level


def gaussian(key, extent, width, bound, shards=(), held_as=jnp.bfloat16):
    entries = jax.random.normal(key, extent, jnp.float32) * width
    if len(shards) > 0:
        entries = level_of(key, extent, shards, -0.22, 0.18) * entries
    return jnp.clip(entries, min=-bound, max=bound).astype(held_as)


def setup_inputs(seed: int = 0) -> dict:
    arg_keys = jax.random.split(jax.random.key(seed), 11)
    return {
        "video_q": draw_video_q(jax.random.fold_in(arg_keys[10], 71), 0),
        "video_k": draw_video_k(jax.random.fold_in(arg_keys[10], 71), 0),
        "video_v": gaussian(arg_keys[2], (TOKENS, WIDTH), 1.0, 6.0, ((0, 32), (1, 8))),
        "audio_q": draw_audio_q(jax.random.fold_in(arg_keys[10], 71), 0),
        "audio_k": draw_audio_k(jax.random.fold_in(arg_keys[10], 71), 0),
        "audio_v": gaussian(arg_keys[5], (AUDIO, WIDTH), 1.0, 6.0, ((0, 32), (1, 8))),
        "video_q_gain": jnp.clip(1.0 + 0.18 * jax.random.normal(arg_keys[6], (WIDTH,), jnp.float32), 0.1, 1.9),
        "audio_k_gain": jnp.clip(1.0 + 0.18 * jax.random.normal(arg_keys[7], (WIDTH,), jnp.float32), 0.1, 1.9),
        "audio_q_gain": jnp.clip(1.0 + 0.18 * jax.random.normal(arg_keys[8], (WIDTH,), jnp.float32), 0.1, 1.9),
        "video_k_gain": jnp.clip(1.0 + 0.18 * jax.random.normal(arg_keys[9], (WIDTH,), jnp.float32), 0.1, 1.9),
    }


EPS = 1e-06

def normalize(rows, gain):
    values = rows.astype(jnp.float32)
    mean_sq = lax.optimization_barrier(jnp.mean(values * values, axis=1, keepdims=True))
    return (values * lax.rsqrt(mean_sq + EPS) * gain.astype(jnp.float32)).astype(jnp.bfloat16)

def reference(video_q, video_k, video_v, audio_q, audio_k, audio_v, video_q_gain, audio_k_gain, audio_q_gain, video_k_gain):
    factor = HD ** (-0.5)
    query_v = normalize(video_q, video_q_gain)
    key_a = normalize(audio_k, audio_k_gain).reshape(AUDIO, HEADS, HD).astype(jnp.float32)
    query_a = normalize(audio_q, audio_q_gain).reshape(AUDIO, HEADS, HD).astype(jnp.float32)
    key_v = normalize(video_k, video_k_gain)
    value_a = audio_v.reshape(AUDIO, HEADS, HD).astype(jnp.float32)
    block = math.gcd(TOKENS, 512)
    count = TOKENS // block

    def first(pair):
        query, value = pair
        scores = jnp.einsum('qhd,khd->hqk', query.reshape(block, HEADS, HD).astype(jnp.float32), key_a) * factor
        top = lax.optimization_barrier(jnp.max(scores, axis=-1, keepdims=True))
        expo = jnp.exp(scores - top)
        total = lax.optimization_barrier(jnp.sum(expo, axis=-1))
        weights = lax.optimization_barrier(expo.astype(jnp.bfloat16)).astype(jnp.float32)
        mixed = jnp.einsum('hqk,khd->qhd', weights, value_a) / jnp.transpose(total)[:, :, None]
        return (value.astype(jnp.float32) + mixed.reshape(block, WIDTH)).astype(jnp.bfloat16)
    video_out = lax.map(first, (query_v.reshape(count, block, WIDTH), video_v.reshape(count, block, WIDTH))).reshape(TOKENS, WIDTH)
    key_blocks = key_v.reshape(N_TOK, TOK_V, HEADS, HD)
    value_blocks = video_out.reshape(N_TOK, TOK_V, HEADS, HD)

    def second(carry, pair):
        run_top, run_out, run_total = carry
        keys, values = pair
        scores = jnp.einsum('qhd,khd->hqk', query_a, keys.astype(jnp.float32)) * factor
        top = lax.optimization_barrier(jnp.max(scores, axis=-1))
        expo = jnp.exp(scores - top[:, :, None])
        total = lax.optimization_barrier(jnp.sum(expo, axis=-1))
        weights = lax.optimization_barrier(expo.astype(jnp.bfloat16)).astype(jnp.float32)
        part = jnp.einsum('hqk,khd->hqd', weights, values.astype(jnp.float32))
        new_top = jnp.maximum(run_top, top)
        old_f = jnp.exp(run_top - new_top)
        new_f = jnp.exp(top - new_top)
        run_out = run_out * old_f[:, :, None] + part * new_f[:, :, None]
        run_total = run_total * old_f + total * new_f
        return ((new_top, run_out, run_total), None)
    start = (jnp.full((HEADS, AUDIO), -1e+30, jnp.float32), jnp.zeros((HEADS, AUDIO, HD), jnp.float32), jnp.zeros((HEADS, AUDIO), jnp.float32))
    (last_top, summed, totals), unused = lax.scan(second, start, (key_blocks, value_blocks))
    result = summed / totals[:, :, None]
    audio_out = jnp.transpose(result, (1, 0, 2)).reshape(AUDIO, WIDTH).astype(jnp.bfloat16)
    return (video_out, audio_out)
```

```python
import functools
import jax
import jax.numpy as jnp
from jax import lax
from jax.experimental import pallas as pl
from jax.experimental.pallas import tpu as pltpu
from jax.sharding import PartitionSpec as P

HEADS = 32
HD = 64
EPS = 1e-06
LOG2E = 1.4426950408889634
NX, NZ, NH = 4, 8, 8
NT = (((1,), (1,)), ((), ()))
BF = jnp.bfloat16
F32 = jnp.float32
MESH = pl.DeviceIdType.MESH
TQ = 256
TK = 512


def make_rhs(q_ref, row0, rows, h, factor):
    pair = pl.multiple_of((h // 2) * 128, 128)
    x = q_ref[pl.ds(row0, rows), pl.ds(pair, 128)].astype(F32) * factor
    lane = lax.broadcasted_iota(jnp.int32, (rows, 128), 1)
    x = jnp.where((lane // HD) == (h % 2), x, 0.0)
    hi = x.astype(BF)
    lo = (x - hi.astype(F32)).astype(BF)
    return jnp.concatenate([hi, lo], axis=1)


def scores_step(k_ref, h, kt, tk, rhs, s_ref, m):
    pair = pl.multiple_of((h // 2) * 128, 128)
    kk = k_ref[pl.ds(kt * tk, tk), pl.ds(pair, 128)]
    s = lax.dot_general(jnp.concatenate([kk, kk], axis=1), rhs, NT, preferred_element_type=F32)
    s_ref[pl.ds(kt * tk, tk), :] = s
    part = jnp.max(s.reshape(tk // 8, 8, s.shape[1]), axis=0)
    return part if m is None else jnp.maximum(m, part)


def mix_step(v_ref, h, kt, tk, s_ref, m, acc):
    p = jnp.exp2(s_ref[pl.ds(kt * tk, tk), :] - m).astype(BF)
    part = jnp.dot(v_ref[h, :, pl.ds(kt * tk, tk)], p, preferred_element_type=F32)
    return part if acc is None else acc + part


def attend(n_items, item, k_ref, v_ref, q_ref, keys, tk, tq, factor, s_refs, m_refs, finish):
    steps = keys // tk

    def scores(i, s_ref, m_ref, mix=None):
        h, row0 = item(i)
        rhs = make_rhs(q_ref, row0, tq, h, factor)
        m, acc = None, None
        for kt in range(steps):
            m = scores_step(k_ref, h, kt, tk, rhs, s_ref, m)
            if mix is not None:
                acc = mix_step(v_ref, mix[0], kt, tk, mix[2], mix[1], acc)
        m_ref[...] = jnp.broadcast_to(jnp.max(m, axis=0, keepdims=True), (8, tq))
        return acc

    def one(i, now, prev):
        h, row0 = item(i - 1)
        mprev = m_refs[prev][0:1]
        acc = scores(i, s_refs[now], m_refs[now], (h, mprev, s_refs[prev]))
        finish(i - 1, h, row0, acc, mprev)

    scores(0, s_refs[0], m_refs[0])

    def body(j, c):
        one(2 * j + 1, 1, 0)
        one(2 * j + 2, 0, 1)
        return c

    lax.fori_loop(0, n_items // 2 - 1, body, 0)
    one(n_items - 1, 1, 0)
    h, row0 = item(n_items - 1)
    mprev = m_refs[1][0:1]
    acc = None
    for kt in range(steps):
        acc = mix_step(v_ref, h, kt, tk, s_refs[1], mprev, acc)
    finish(n_items - 1, h, row0, acc, mprev)


def row_sums(x):
    x = x.astype(F32)
    y = x[:, :128] * x[:, :128] + x[:, 128:] * x[:, 128:]
    return jnp.sum(jnp.transpose(y), axis=0, keepdims=True)


def along_rows(row):
    return jnp.transpose(jnp.broadcast_to(row, (128, 128)))


def scaled(x, col, gain):
    c = jnp.concatenate([col, col], axis=1)
    return (x.astype(F32) * c * gain).astype(BF)


def kernel(vq_h, vk_h, vv_h, aq_h, ak_h, av_h, gvq, gak, gaq, gvk, vout_h, aout,
           vq, vk, vv, araw, va, ka, qa, vT, voT, vvT, sa, sb, ma, mb,
           st_own, st_all, pT, xrecv, lse, lrecv, zsend, zrecv, lsend, lzrecv, vout,
           in_sem, out_sem, st_send, st_recv, g_send, g_recv, x_send, x_recv, xl_send, xl_recv, z_send, z_recv, zl_send, zl_recv):
    hx = lax.axis_index("heads")
    tok = lax.axis_index("tok")
    x0, z0 = tok // NZ, tok % NZ
    n, na, ar = vq.shape[0], ka.shape[0], araw.shape[1]

    def at(x, z):
        return (x % NX) * NZ + (z % NZ)

    ins = [pltpu.make_async_copy(vq_h, vq, in_sem.at[0]), pltpu.make_async_copy(vk_h, vk, in_sem.at[1]),
           pltpu.make_async_copy(aq_h, araw.at[1], in_sem.at[2]), pltpu.make_async_copy(ak_h, araw.at[0], in_sem.at[3]),
           pltpu.make_async_copy(av_h, va.at[pl.ds(pl.multiple_of(tok * ar, ar), ar)], in_sem.at[4]),
           pltpu.make_async_copy(vv_h, vv, in_sem.at[5])]
    for c in ins:
        c.start()

    peers = [{"heads": (hx + i) % NH} for i in range(1, NH)]
    peers += [{"tok": at(x0 + i, z0)} for i in range(1, NX)] + [{"tok": at(x0, z0 + i)} for i in range(1, NZ)]
    barrier = pltpu.get_barrier_semaphore()
    for p in peers:
        pl.semaphore_signal(barrier, inc=1, device_id=p, device_id_type=MESH)
    pl.semaphore_wait(barrier, len(peers))

    def gather(buf, t, zfirst):
        np_, ns = (NZ, NX) if zfirst else (NX, NZ)
        p0, s0 = (z0, x0) if zfirst else (x0, z0)

        def dev(p, s):
            return at(s, p) if zfirst else at(p, s)

        def block(b):
            return buf.at[pl.ds(pl.multiple_of(b * ar, ar), ar)]

        def send(b, to):
            pltpu.make_async_remote_copy(src_ref=block(b), dst_ref=block(b), send_sem=g_send.at[t], recv_sem=g_recv.at[t, b],
                                         device_id={"tok": to}, device_id_type=MESH).start()

        def recv(b):
            pltpu.make_async_copy(block(b), block(b), g_recv.at[t, b]).wait()

        def spread(p):
            send(dev(p, s0), dev(p0, s0 + 1))
            send(dev(p, s0), dev(p0, s0 - 1))

        half, shalf = np_ // 2, ns // 2
        sgn_s = 1 - 2 * (s0 % 2)
        steps = []

        def first():
            send(dev(p0, s0), dev(p0 + 1, s0))
            send(dev(p0, s0), dev(p0 - 1, s0))
            spread(p0)

        steps.append(first)
        for i in range(1, half):
            def prim(i=i):
                for d in (1, -1):
                    b = dev(p0 - d * i, s0)
                    recv(b)
                    if i < half - 1:
                        send(b, dev(p0 + d, s0))
                if i == half - 1:
                    send(dev(p0 - sgn_s * i, s0), dev(p0 + sgn_s, s0))
                for d in (1, -1):
                    spread(p0 - d * i)
            steps.append(prim)

        def opposite():
            recv(dev(p0 + half, s0))
            spread(p0 + half)

        steps.append(opposite)
        order = [0] + [o for i in range(1, half) for o in (-i, i)] + [half]
        for j in range(1, shalf):
            for o in order:
                def sec(o=o, j=j):
                    p = p0 + o
                    for d in (1, -1):
                        b = dev(p, s0 - d * j)
                        recv(b)
                        if j < shalf - 1:
                            send(b, dev(p0, s0 + d))
                    if j == shalf - 1:
                        d = 1 - 2 * ((p0 + o + np_) % 2)
                        send(dev(p, s0 - d * j), dev(p0, s0 + d))
                steps.append(sec)
        for o in order:
            steps.append(lambda o=o: recv(dev(p0 + o, s0 + shalf)))
        return steps

    def drain(buf, t):
        rows = buf.at[pl.ds(0, (NX * NZ - 1) * ar)]
        pltpu.make_async_copy(rows, rows, g_send.at[t]).wait()

    ins[4].wait()
    gv = gather(va, 0, True)
    gv[0]()

    st_own[...] = jnp.zeros_like(st_own)
    for i, ref in ((0, vq), (1, vk)):
        ins[i].wait()
        for c in range(n // 128):
            st_own[i * 8 + c:i * 8 + c + 1, :] = row_sums(ref[c * 128:(c + 1) * 128, :])
    ins[2].wait()
    ins[3].wait()
    st_own[16:17, :] = row_sums(araw[...].reshape(2 * ar, 256))
    st_copies = []
    for i in range(1, NH):
        c = pltpu.make_async_remote_copy(src_ref=st_own, dst_ref=st_all.at[i - 1], send_sem=st_send.at[i - 1], recv_sem=st_recv.at[i - 1],
                                         device_id={"heads": (hx + i) % NH}, device_id_type=MESH)
        c.start()
        st_copies.append(c)
    for s in gv[1:3]:
        s()
    for c in st_copies:
        c.wait()
    total = st_own[...]
    for i in range(NH - 1):
        total = total + st_all[i]
    scale = lax.rsqrt(total * (1.0 / (HEADS * HD)) + EPS)
    col = along_rows(scale[16:17])
    mine = pl.ds(pl.multiple_of(tok * ar, ar), ar)
    ka[mine, :] = scaled(araw[0], col[0:ar], gak[...])
    qa[mine, :] = scaled(araw[1], col[ar:2 * ar], gaq[...])
    gk = gather(ka, 1, False)
    gq = gather(qa, 2, True)
    gk[0]()
    for s in gv[3:5]:
        s()
    for c in range(n // 128):
        vq[c * 128:(c + 1) * 128, :] = scaled(vq[c * 128:(c + 1) * 128, :], along_rows(scale[c:c + 1]), gvq[...])
        vk[c * 128:(c + 1) * 128, :] = scaled(vk[c * 128:(c + 1) * 128, :], along_rows(scale[8 + c:9 + c]), gvk[...])
    ins[5].wait()
    for c in range(0, n, 256):
        t = jnp.transpose(vv[c:c + 256, :])
        for h in range(4):
            vvT[h, :, c:c + 256] = t[h * HD:(h + 1) * HD]
            voT[h, HD:HD + 16, c:c + 256] = jnp.ones((16, 256), BF)
    rest = [gv[5:], gk[1:]]
    for i in range(max(map(len, rest))):
        for r in rest:
            if i < len(r):
                r[i]()
    for s in gq:
        s()
    for c in range(0, na, 256):
        t = jnp.transpose(va[c:c + 256, :])
        for h in range(4):
            vT[h, 0:HD, c:c + 256] = t[h * HD:(h + 1) * HD]
            vT[h, HD:HD + 16, c:c + 256] = jnp.ones((16, 256), BF)

    factor = HD ** (-0.5) * LOG2E

    def finish1(i, h, row0, acc, m):
        o = acc[0:HD] * (1.0 / acc[HD:HD + 1])
        r = vvT[h, :, pl.ds(row0, TQ)].astype(F32) + o
        voT[h, 0:HD, pl.ds(row0, TQ)] = r.astype(BF)

    attend(4 * (n // TQ), lambda i: (i % 4, pl.multiple_of((i // 4) * TQ, TQ)), ka, vT, vq, na, TK, TQ, factor, (sa, sb), (ma, mb), finish1)
    for c in range(0, n, 256):
        t = jnp.concatenate([voT[h, 0:HD, c:c + 256] for h in range(4)], axis=0)
        vout[c:c + 256, :] = jnp.transpose(t)
    out_copy = pltpu.make_async_copy(vout, vout_h, out_sem)
    out_copy.start()

    slab = na // NX
    per = 4 * (slab // TQ)

    def sl(k):
        return (x0 + (2, 1, 3, 0)[k]) % NX

    x_copies = []
    for k in range(NX):
        xs = sl(k)

        def finish2(i, h, row0, acc, m, k=k, xs=xs):
            o = acc[0:HD] * (1.0 / acc[HD:HD + 1])
            off = pl.multiple_of(row0 - xs * slab, TQ)
            pT[k, pl.ds(pl.multiple_of(h * HD, HD), HD), pl.ds(off, TQ)] = o.astype(BF)
            lse[k, pl.ds(h, 1), pl.ds(off, TQ)] = m + jnp.log2(acc[HD:HD + 1])

        attend(per, lambda i, xs=xs: (i % 4, pl.multiple_of(xs * slab + (i // 4) * TQ, TQ)), vk, voT, qa, n, TK, TQ, factor, (sa, sb), (ma, mb), finish2)
        if k < 3:
            a = pltpu.make_async_remote_copy(src_ref=pT.at[k], dst_ref=xrecv.at[k], send_sem=x_send.at[k], recv_sem=x_recv.at[k],
                                             device_id={"tok": at(xs, z0)}, device_id_type=MESH)
            b = pltpu.make_async_remote_copy(src_ref=lse.at[k], dst_ref=lrecv.at[k], send_sem=xl_send.at[k], recv_sem=xl_recv.at[k],
                                             device_id={"tok": at(xs, z0)}, device_id_type=MESH)
            a.start()
            b.start()
            x_copies += [a, b]
    for c in x_copies:
        c.wait()
    ls = [lrecv[k] for k in range(3)] + [lse[3]]
    top = functools.reduce(jnp.maximum, [l[0:4] for l in ls])
    ws = [jnp.exp2(l[0:4] - top) for l in ls]
    tot = ws[0] + ws[1] + ws[2] + ws[3]
    inv = 1.0 / tot
    lsend[0:4, :] = top + jnp.log2(tot)
    lsend[4:8, :] = jnp.zeros((4, slab), F32)
    ws = [w * inv for w in ws]
    for c in range(0, slab, 256):
        parts = []
        for h in range(4):
            o = pT[3, h * HD:(h + 1) * HD, c:c + 256].astype(F32) * ws[3][h:h + 1, c:c + 256]
            for k in range(3):
                o = o + xrecv[k, h * HD:(h + 1) * HD, c:c + 256].astype(F32) * ws[k][h:h + 1, c:c + 256]
            parts.append(o.astype(BF))
        zsend[c:c + 256, :] = jnp.transpose(jnp.concatenate(parts, axis=0))
    z_copies = []
    for i in range(1, NZ):
        zt = (z0 + i) % NZ
        a = pltpu.make_async_remote_copy(src_ref=zsend.at[pl.ds(pl.multiple_of(zt * ar, ar), ar)], dst_ref=zrecv.at[i - 1],
                                         send_sem=z_send.at[i - 1], recv_sem=z_recv.at[i - 1], device_id={"tok": at(x0, zt)}, device_id_type=MESH)
        b = pltpu.make_async_remote_copy(src_ref=lsend.at[:, pl.ds(pl.multiple_of((zt // 2) * 128, 128), 128)], dst_ref=lzrecv.at[i - 1],
                                         send_sem=zl_send.at[i - 1], recv_sem=zl_recv.at[i - 1], device_id={"tok": at(x0, zt)}, device_id_type=MESH)
        a.start()
        b.start()
        z_copies += [a, b]
    for c in z_copies:
        c.wait()
    ls = [lzrecv[i] for i in range(NZ - 1)] + [lsend[:, pl.ds(pl.multiple_of((z0 // 2) * 128, 128), 128)]]
    top = functools.reduce(jnp.maximum, ls)
    ws = [jnp.exp2(l - top) for l in ls]
    inv = 1.0 / functools.reduce(jnp.add, ws)
    odd = (z0 % 2) == 1
    acc = jnp.zeros((ar, 256), F32)
    for i in range(NZ):
        w = ws[i] * inv
        cols = []
        for h in range(4):
            t = jnp.transpose(jnp.broadcast_to(w[h:h + 1], (128, 128)))
            cols.append(jnp.where(odd, t[ar:2 * ar, 0:HD], t[0:ar, 0:HD]))
        wide = jnp.concatenate(cols, axis=1)
        o = zrecv[i] if i < NZ - 1 else zsend[pl.ds(pl.multiple_of(z0 * ar, ar), ar), :]
        acc = acc + o.astype(F32) * wide
    aout[...] = acc.astype(BF)
    for b, t in ((va, 0), (ka, 1), (qa, 2)):
        drain(b, t)
    out_copy.wait()


def body(video_q, video_k, video_v, audio_q, audio_k, audio_v, video_q_gain, audio_k_gain, audio_q_gain, video_k_gain):
    n, w = video_q.shape
    ar = audio_q.shape[0]
    na = ar * NX * NZ
    slab = na // NX
    A = pl.BlockSpec(memory_space=pl.ANY)
    V = pl.BlockSpec(memory_space=pltpu.VMEM)
    M = pltpu.VMEM
    D = pltpu.SemaphoreType.DMA
    return pl.pallas_call(
        kernel,
        out_shape=(jax.ShapeDtypeStruct((n, w), BF), jax.ShapeDtypeStruct((ar, w), BF)),
        in_specs=[A] * 6 + [V] * 4,
        out_specs=(A, V),
        scratch_shapes=[
            M((n, w), BF), M((n, w), BF), M((n, w), BF), M((2, ar, w), BF), M((na, w), BF), M((na, w), BF), M((na, w), BF),
            M((4, HD + 16, na), BF), M((4, HD + 16, n), BF), M((4, HD, n), BF),
            M((na, TQ), F32), M((na, TQ), F32), M((8, TQ), F32), M((8, TQ), F32),
            M((24, 128), F32), M((NH - 1, 24, 128), F32),
            M((NX, w, slab), BF), M((3, w, slab), BF), M((NX, 8, slab), F32), M((3, 8, slab), F32),
            M((slab, w), BF), M((NZ - 1, ar, w), BF), M((8, slab), F32), M((NZ - 1, 8, 128), F32), M((n, w), BF),
            D((6,)), D, D((NH - 1,)), D((NH - 1,)), D((3,)), D((3, NX * NZ)),
            D((3,)), D((3,)), D((3,)), D((3,)), D((NZ - 1,)), D((NZ - 1,)), D((NZ - 1,)), D((NZ - 1,)),
        ],
        compiler_params=pltpu.CompilerParams(collective_id=0, has_side_effects=True, vmem_limit_bytes=60 * 2**20),
        name="av_cross",
    )(video_q, video_k, video_v, audio_q, audio_k, audio_v, video_q_gain[None], audio_k_gain[None], audio_q_gain[None], video_k_gain[None])


def solution(mesh):
    return jax.shard_map(
        body,
        mesh=mesh,
        in_specs=(P("tok", "heads"),) * 6 + (P("heads"),) * 4,
        out_specs=(P("tok", "heads"), P("tok", "heads")),
        check_vma=False,
    )
```

```python
import functools
import heapq
import jax
import jax.numpy as jnp
from jax import lax
from jax.experimental import pallas as pl
from jax.experimental.pallas import tpu as pltpu
from jax.sharding import PartitionSpec as P

HEADS = 32
HD = 64
EPS = 1e-06
LOG2E = 1.4426950408889634
NX, NZ, NH = 4, 8, 8
NT = (((1,), (1,)), ((), ()))
BF = jnp.bfloat16
F32 = jnp.float32
MESH = pl.DeviceIdType.MESH
TQ = 256
TK = 512

SCHEME = (1, 1, 0, 1, 1, 1)
BLOCK_US, HOP_US, LATE_US = 0.352, 3.3, 2.7


def plan():
    items = len(SCHEME)

    def signed(v, n):
        return v if v <= n // 2 else v - n

    def onward(key):
        t, dx, dz = key
        np_, ns = (NZ, NX) if SCHEME[t] else (NX, NZ)
        p, s = (signed(dz, NZ), signed(dx, NX)) if SCHEME[t] else (signed(dx, NX), signed(dz, NZ))
        hp, hs = np_ // 2, ns // 2
        out = []
        if s == 0:
            if p == 0:
                out += [("p", 1), ("p", -1)]
            elif abs(p) < hp - 1 or p == 1 - hp:
                out.append(("p", -1 if p > 0 else 1))
            out += [("s", 1), ("s", -1)]
        elif abs(s) < hs - 1 or (abs(s) == hs - 1 and (s < 0) == (p % 2 == 0)):
            out.append(("s", -1 if s > 0 else 1))
        return p, s, out

    queue, busy, events, order, count = {}, {}, [], [], 0
    for t in range(items):
        heapq.heappush(events, (0.0 if t < 2 else LATE_US, t, 0, (t, 0, 0)))
    count = items
    while events:
        now, _, kind, x = heapq.heappop(events)
        if kind == 0:
            p, s, out = onward(x)
            for a, d in out:
                link = ("z" if (a == "p") == bool(SCHEME[x[0]]) else "x", d)
                count += 2
                heapq.heappush(queue.setdefault(link, []), (int(x[0] >= 4), int(a == "s"), now, count, x, p, s, a, d))
                heapq.heappush(events, (max(now, busy.get(link, 0.0)), count + 1, 1, link))
        elif queue.get(x):
            if now < busy.get(x, 0.0) - 1e-9:
                count += 1
                heapq.heappush(events, (busy[x], count, 1, x))
                continue
            _, _, _, _, key, p, s, a, d = heapq.heappop(queue[x])
            even_p, even_s = 1 - 2 * (p % 2), 1 - 2 * (s % 2)
            order.append((key[0], even_s * p, even_p * s, a, d * (1 if a == "p" else even_p), now))
            busy[x] = now + BLOCK_US
            t, dx, dz = key
            landed = (t, dx, (dz - x[1]) % NZ) if x[0] == "z" else (t, (dx - x[1]) % NX, dz)
            count += 1
            heapq.heappush(events, (now + BLOCK_US + HOP_US, count, 0, landed))
            count += 1
            heapq.heappush(events, (busy[x], count, 1, x))
    assert len(order) == items * (NX * NZ - 1)
    return order


def make_rhs(x, h, factor):
    x = x.astype(F32) * factor
    lane = lax.broadcasted_iota(jnp.int32, x.shape, 1)
    x = jnp.where((lane // HD) == (h % 2), x, 0.0)
    hi = x.astype(BF)
    lo = (x - hi.astype(F32)).astype(BF)
    return jnp.concatenate([hi, lo], axis=1)


def pair_of(h):
    return pl.ds(pl.multiple_of((h // 2) * 128, 128), 128)


def scores_step(k_ref, h, kt, tk, rhs, s_ref, m):
    pair = pl.multiple_of((h // 2) * 128, 128)
    kk = k_ref[pl.ds(kt * tk, tk), pl.ds(pair, 128)]
    s = lax.dot_general(jnp.concatenate([kk, kk], axis=1), rhs, NT, preferred_element_type=F32)
    s_ref[pl.ds(kt * tk, tk), :] = s
    part = jnp.max(s.reshape(tk // 8, 8, s.shape[1]), axis=0)
    return part if m is None else jnp.maximum(m, part)


def mix_step(v_ref, h, kt, tk, s_ref, m, acc):
    p = jnp.exp2(s_ref[pl.ds(kt * tk, tk), :] - m).astype(BF)
    part = jnp.dot(v_ref[h, :, pl.ds(kt * tk, tk)], p, preferred_element_type=F32)
    return part if acc is None else acc + part


class Pipe:
    def __init__(self, item, k_ref, v_ref, keys, factor, s_refs, m_refs, finish):
        self.item, self.k, self.v, self.keys, self.factor = item, k_ref, v_ref, keys, factor
        self.s, self.m, self.finish = s_refs, m_refs, finish

    def scores(self, i, now, mix=None):
        h, x = self.item(i)
        rhs = make_rhs(x, h, self.factor)
        m, acc = None, None
        for kt in range(self.keys // TK):
            m = scores_step(self.k, h, kt, TK, rhs, self.s[now], m)
            if mix is not None:
                acc = mix_step(self.v, mix[0], kt, TK, self.s[1 - now], mix[1], acc)
        self.m[now][...] = jnp.broadcast_to(jnp.max(m, axis=0, keepdims=True), (8, TQ))
        return acc

    def one(self, i, now):
        prev = self.m[1 - now][0:1]
        h = (i - 1) % 4
        acc = self.scores(i, now, (h, prev))
        self.finish(i - 1, h, acc, prev)

    def last(self, i, now):
        prev = self.m[now][0:1]
        h = i % 4
        acc = None
        for kt in range(self.keys // TK):
            acc = mix_step(self.v, h, kt, TK, self.s[now], prev, acc)
        self.finish(i, h, acc, prev)


def row_sums(x):
    x = x.astype(F32)
    y = x[:, :128] * x[:, :128] + x[:, 128:] * x[:, 128:]
    return jnp.sum(jnp.transpose(y), axis=0, keepdims=True)


def along_rows(row):
    return jnp.transpose(jnp.broadcast_to(row, (128, 128)))


def scaled(x, col, gain):
    c = jnp.concatenate([col, col], axis=1)
    return (x.astype(F32) * c * gain).astype(BF)


def kernel(vq_h, vk_h, vv_h, aq_h, ak_h, av_h, gvq_h, gak_h, gaq_h, gvk_h, vout_h, aout,
           vq, vk, vv, gains, araw, va, ka, qa, vT, voT, vvT, sa, sb, ma, mb,
           sta_own, sta_all, st_own, st_all, pT, xrecv, lse, lrecv, zsend, zrecv, lsend, lzrecv, vout,
           in_sem, out_sem, sta_send, sta_recv, st_send, st_recv, g_send, g_recv, x_send, x_recv, xl_send, xl_recv, z_send, z_recv, zl_send, zl_recv):
    hx = lax.axis_index("heads")
    tok = lax.axis_index("tok")
    x0, z0 = tok // NZ, tok % NZ
    n, na, ar = vq.shape[0], ka.shape[0], araw.shape[1]

    def at(x, z):
        return (x % NX) * NZ + (z % NZ)

    ins = [pltpu.make_async_copy(vq_h, vq, in_sem.at[0]), pltpu.make_async_copy(vk_h, vk, in_sem.at[1]),
           pltpu.make_async_copy(aq_h, araw.at[1], in_sem.at[2]), pltpu.make_async_copy(ak_h, araw.at[0], in_sem.at[3]),
           pltpu.make_async_copy(av_h, va.at[pl.ds(pl.multiple_of(tok * ar, ar), ar)], in_sem.at[4]),
           pltpu.make_async_copy(vv_h, vv, in_sem.at[5])]
    ins += [pltpu.make_async_copy(g, gains.at[i], in_sem.at[6 + i]) for i, g in enumerate((gvq_h, gak_h, gaq_h, gvk_h))]
    for i in (2, 3, 4, 0, 1, 6, 7, 8, 9, 5):
        ins[i].start()

    peers = [{"heads": (hx + i) % NH} for i in range(1, NH)]
    peers += [{"tok": at(x0 + i, z0)} for i in range(1, NX)] + [{"tok": at(x0, z0 + i)} for i in range(1, NZ)]
    barrier = pltpu.get_barrier_semaphore()
    for p in peers:
        pl.semaphore_signal(barrier, inc=1, device_id=p, device_id_type=MESH)
    sta_own[...] = jnp.zeros_like(sta_own)
    ins[2].wait()
    ins[3].wait()
    sta_own[0:1, :] = row_sums(araw[...].reshape(2 * ar, 256))
    ins[4].wait()
    pl.semaphore_wait(barrier, len(peers))

    half = ar // 2
    bufs = (va, va, ka, ka, qa, qa)
    odd_x, odd_z = 1 - 2 * (x0 % 2), 1 - 2 * (z0 % 2)
    order = plan()
    waited = {(t, 0, 0) for t in range(6)}

    def source(t, p, s):
        zf = SCHEME[t]
        sp = (odd_x if zf else odd_z) * (1 - 2 * (s % 2))
        ss = (odd_z if zf else odd_x) * (1 - 2 * (p % 2))
        po, so = sp * p, ss * s
        return at(x0 + so, z0 + po) if zf else at(x0 + po, z0 + so)

    def piece(t, b):
        return bufs[t].at[pl.ds(pl.multiple_of(b * ar + (t % 2) * half, half), half)]

    def arrived(t, p, s):
        np_, ns = (NZ, NX) if SCHEME[t] else (NX, NZ)
        if p == -(np_ // 2):
            p = np_ // 2
        if s == -(ns // 2):
            s = ns // 2
        if (t, p, s) not in waited:
            waited.add((t, p, s))
            b = source(t, p, s)
            ref = piece(t, b)
            pltpu.make_async_copy(ref, ref, g_recv.at[t, b]).wait()

    done = [0]

    def pump(until=None, upto=None):
        while done[0] < len(order):
            t, p, s, a, d, when = order[done[0]]
            if (until is not None and when > until) or (upto is not None and done[0] >= upto):
                return
            arrived(t, p, s)
            zf = SCHEME[t]
            sign = (odd_x if zf else odd_z) if a == "p" else (odd_z if zf else odd_x) * (1 - 2 * (p % 2))
            step = sign * d
            to = at(x0, z0 + step) if (a == "p") == bool(zf) else at(x0 + step, z0)
            b = source(t, p, s)
            ref = piece(t, b)
            pltpu.make_async_remote_copy(src_ref=ref, dst_ref=ref, send_sem=g_send.at[t], recv_sem=g_recv.at[t, b],
                                         device_id={"tok": to}, device_id_type=MESH).start()
            done[0] += 1

    def complete(ts):
        for t in ts:
            np_, ns = (NZ, NX) if SCHEME[t] else (NX, NZ)
            for p in range(1 - np_ // 2, np_ // 2 + 1):
                for s in range(1 - ns // 2, ns // 2 + 1):
                    arrived(t, p, s)

    def to_heads(own, every, send, recv):
        out = []
        for i in range(1, NH):
            c = pltpu.make_async_remote_copy(src_ref=own, dst_ref=every.at[i - 1], send_sem=send.at[i - 1], recv_sem=recv.at[i - 1],
                                             device_id={"heads": (hx + i) % NH}, device_id_type=MESH)
            c.start()
            out.append(c)
        return out

    def scale_of(copies, own, every):
        for c in copies:
            c.wait()
        total = own[...]
        for i in range(NH - 1):
            total = total + every[i]
        return lax.rsqrt(total * (1.0 / (HEADS * HD)) + EPS)

    a_copies = to_heads(sta_own, sta_all, sta_send, sta_recv)
    pump(until=0.1)
    for i, ref in ((0, vq), (1, vk)):
        ins[i].wait()
        for c in range(n // 128):
            st_own[i * 8 + c:i * 8 + c + 1, :] = row_sums(ref[c * 128:(c + 1) * 128, :])
    v_copies = to_heads(st_own, st_all, st_send, st_recv)
    for i in range(6, 10):
        ins[i].wait()
    col = along_rows(scale_of(a_copies, sta_own, sta_all)[0:1])
    mine = pl.ds(pl.multiple_of(tok * ar, ar), ar)
    ka[mine, :] = scaled(araw[0], col[0:ar], gains[1])
    qa[mine, :] = scaled(araw[1], col[ar:2 * ar], gains[2])
    pump(until=LATE_US + 0.4)
    ins[5].wait()
    for c in range(0, n, 256):
        t = jnp.transpose(vv[c:c + 256, :])
        for h in range(4):
            vvT[h, :, c:c + 256] = t[h * HD:(h + 1) * HD]
            voT[h, HD:HD + 16, c:c + 256] = jnp.ones((16, 256), BF)
    pump(until=LATE_US + 1.0)
    scale = scale_of(v_copies, st_own, st_all)
    factor = HD ** (-0.5) * LOG2E
    for qt in range(n // TQ):
        for c in range(qt * TQ // 128, (qt + 1) * TQ // 128):
            vq[c * 128:(c + 1) * 128, :] = scaled(vq[c * 128:(c + 1) * 128, :], along_rows(scale[c:c + 1]), gains[0])
        pump(until=LATE_US + 1.6 + 0.6 * qt)
    for c in range(n // 128):
        vk[c * 128:(c + 1) * 128, :] = scaled(vk[c * 128:(c + 1) * 128, :], along_rows(scale[8 + c:9 + c]), gains[3])

    pump(upto=1 + max(i for i, o in enumerate(order) if o[0] < 4))
    complete((0, 1))
    for c in range(0, na, 256):
        t = jnp.transpose(va[c:c + 256, :])
        for h in range(4):
            vT[h, 0:HD, c:c + 256] = t[h * HD:(h + 1) * HD]
            vT[h, HD:HD + 16, c:c + 256] = jnp.ones((16, 256), BF)
    complete((2, 3))

    def item1(i):
        return i % 4, vq[(i // 4) * TQ:(i // 4 + 1) * TQ, (i % 4 // 2) * 128:(i % 4 // 2 + 1) * 128]

    def finish1(i, h, acc, m):
        r0 = (i // 4) * TQ
        o = acc[0:HD] * (1.0 / acc[HD:HD + 1])
        voT[h, 0:HD, r0:r0 + TQ] = (vvT[h, :, r0:r0 + TQ].astype(F32) + o).astype(BF)

    one = Pipe(item1, ka, vT, na, factor, (sa, sb), (ma, mb), finish1)
    n1 = 4 * (n // TQ)
    left = len(order) - done[0]
    start = done[0]
    one.scores(0, 0)
    for i in range(1, n1):
        pump(upto=start + (left * i) // (n1 - 4))
        one.one(i, i % 2)
    one.last(n1 - 1, (n1 - 1) % 2)
    pump()
    complete((4, 5))

    slab = na // NX

    def slab_of(k):
        o = jnp.where(k == 0, 2, jnp.where(k == 1, 1, jnp.where(k == 2, 3, 0)))
        return (x0 + o) % NX

    def item2(i):
        h, k, hh = i % 4, (i // 4) % 4, i // 16
        base = slab_of(k) * slab + hh * ar
        x = [qa[pl.ds(pl.multiple_of(base + 2 * j * ar, ar), ar), pair_of(h)] for j in range(4)]
        return h, jnp.concatenate(x, axis=0)

    def finish2(i, h, acc, m):
        p = i // 4
        o = acc[0:HD] * (1.0 / acc[HD:HD + 1])
        pT[p, pl.ds(pl.multiple_of(h * HD, HD), HD), :] = o.astype(BF)
        lse[p, pl.ds(h, 1), :] = m + jnp.log2(acc[HD:HD + 1])

    def x_pair(p, k, to):
        a = pltpu.make_async_remote_copy(src_ref=pT.at[p], dst_ref=xrecv.at[p], send_sem=x_send.at[p], recv_sem=x_recv.at[p],
                                         device_id={"tok": at(to, z0)}, device_id_type=MESH)
        b = pltpu.make_async_remote_copy(src_ref=lse.at[p], dst_ref=lrecv.at[p], send_sem=xl_send.at[p], recv_sem=xl_recv.at[p],
                                         device_id={"tok": at(to, z0)}, device_id_type=MESH)
        return a, b

    two = Pipe(item2, vk, voT, n, factor, (sa, sb), (ma, mb), finish2)
    two.scores(0, 0)

    def trip(p, c):
        for j in range(4):
            two.one(4 * p + j + 1, (j + 1) % 2)

        @pl.when(p % 4 < 3)
        def _():
            for c_ in x_pair(p, p % 4, slab_of(p % 4)):
                c_.start()

        return c

    lax.fori_loop(0, 7, trip, 0)
    for j in range(3):
        two.one(29 + j, (j + 1) % 2)
    two.last(31, 1)

    for c in range(0, n, 256):
        t = jnp.concatenate([voT[h, 0:HD, c:c + 256] for h in range(4)], axis=0)
        vout[c:c + 256, :] = jnp.transpose(t)
    out_copy = pltpu.make_async_copy(vout, vout_h, out_sem)
    out_copy.start()

    def z_pair(i):
        zt = (z0 + i) % NZ
        hh, j = zt % 2, zt // 2
        a = pltpu.make_async_remote_copy(src_ref=zsend.at[hh, pl.ds(pl.multiple_of(j * ar, ar), ar)], dst_ref=zrecv.at[i - 1],
                                         send_sem=z_send.at[i - 1], recv_sem=z_recv.at[i - 1], device_id={"tok": at(x0, zt)}, device_id_type=MESH)
        b = pltpu.make_async_remote_copy(src_ref=lsend.at[hh, :, pl.ds(pl.multiple_of((j // 2) * 128, 128), 128)], dst_ref=lzrecv.at[i - 1],
                                         send_sem=zl_send.at[i - 1], recv_sem=zl_recv.at[i - 1], device_id={"tok": at(x0, zt)}, device_id_type=MESH)
        return a, b

    for hh in range(2):
        for k in range(3):
            for c in x_pair(hh * 4 + k, k, slab_of(k)):
                c.wait()
        ls = [lrecv[hh * 4 + k] for k in range(3)] + [lse[hh * 4 + 3]]
        top = functools.reduce(jnp.maximum, [l[0:4] for l in ls])
        ws = [jnp.exp2(l[0:4] - top) for l in ls]
        tot = ws[0] + ws[1] + ws[2] + ws[3]
        inv = 1.0 / tot
        lsend[hh, 0:4, :] = top + jnp.log2(tot)
        lsend[hh, 4:8, :] = jnp.zeros((4, TQ), F32)
        ws = [w * inv for w in ws]
        parts = []
        for h in range(4):
            o = pT[hh * 4 + 3, h * HD:(h + 1) * HD, :].astype(F32) * ws[3][h:h + 1]
            for k in range(3):
                o = o + xrecv[hh * 4 + k, h * HD:(h + 1) * HD, :].astype(F32) * ws[k][h:h + 1]
            parts.append(o.astype(BF))
        zsend[hh] = jnp.transpose(jnp.concatenate(parts, axis=0))
        for j in range(4):
            i = 2 * j + 2 - (z0 + hh) % 2

            @pl.when(i < NZ)
            def _():
                for c in z_pair(i):
                    c.start()

    for i in range(1, NZ):
        for c in z_pair(i):
            c.wait()
    own = z0 % 2
    ls = [lzrecv[i] for i in range(NZ - 1)] + [lsend[own, :, pl.ds(pl.multiple_of((z0 // 4) * 128, 128), 128)]]
    top = functools.reduce(jnp.maximum, ls)
    ws = [jnp.exp2(l - top) for l in ls]
    inv = 1.0 / functools.reduce(jnp.add, ws)
    odd = ((z0 // 2) % 2) == 1
    acc = jnp.zeros((ar, 256), F32)
    for i in range(NZ):
        w = ws[i] * inv
        cols = []
        for h in range(4):
            t = jnp.transpose(jnp.broadcast_to(w[h:h + 1], (128, 128)))
            cols.append(jnp.where(odd, t[ar:2 * ar, 0:HD], t[0:ar, 0:HD]))
        wide = jnp.concatenate(cols, axis=1)
        o = zrecv[i] if i < NZ - 1 else zsend[own, pl.ds(pl.multiple_of((z0 // 2) * ar, ar), ar), :]
        acc = acc + o.astype(F32) * wide
    aout[...] = acc.astype(BF)
    for t in range(6):
        rows = bufs[t].at[pl.ds(0, (NX * NZ - 1) * half)]
        pltpu.make_async_copy(rows, rows, g_send.at[t]).wait()
    out_copy.wait()


def body(video_q, video_k, video_v, audio_q, audio_k, audio_v, video_q_gain, audio_k_gain, audio_q_gain, video_k_gain):
    n, w = video_q.shape
    ar = audio_q.shape[0]
    na = ar * NX * NZ
    A = pl.BlockSpec(memory_space=pl.ANY)
    V = pl.BlockSpec(memory_space=pltpu.VMEM)
    M = pltpu.VMEM
    D = pltpu.SemaphoreType.DMA
    return pl.pallas_call(
        kernel,
        out_shape=(jax.ShapeDtypeStruct((n, w), BF), jax.ShapeDtypeStruct((ar, w), BF)),
        in_specs=[A] * 10,
        out_specs=(A, V),
        scratch_shapes=[
            M((n, w), BF), M((n, w), BF), M((n, w), BF), M((4, 1, w), F32), M((2, ar, w), BF), M((na, w), BF), M((na, w), BF), M((na, w), BF),
            M((4, HD + 16, na), BF), M((4, HD + 16, n), BF), M((4, HD, n), BF),
            M((na, TQ), F32), M((na, TQ), F32), M((8, TQ), F32), M((8, TQ), F32),
            M((8, 128), F32), M((NH - 1, 8, 128), F32), M((16, 128), F32), M((NH - 1, 16, 128), F32),
            M((8, w, TQ), BF), M((8, w, TQ), BF), M((8, 8, TQ), F32), M((8, 8, TQ), F32),
            M((2, TQ, w), BF), M((NZ - 1, ar, w), BF), M((2, 8, TQ), F32), M((NZ - 1, 8, 128), F32), M((n, w), BF),
            D((10,)), D, D((NH - 1,)), D((NH - 1,)), D((NH - 1,)), D((NH - 1,)), D((6,)), D((6, NX * NZ)),
            D((8,)), D((8,)), D((8,)), D((8,)), D((NZ - 1,)), D((NZ - 1,)), D((NZ - 1,)), D((NZ - 1,)),
        ],
        compiler_params=pltpu.CompilerParams(collective_id=0, has_side_effects=True, vmem_limit_bytes=60 * 2**20),
        name="av_cross",
    )(video_q, video_k, video_v, audio_q, audio_k, audio_v, video_q_gain[None], audio_k_gain[None], audio_q_gain[None], video_k_gain[None])


def solution(mesh):
    return jax.shard_map(
        body,
        mesh=mesh,
        in_specs=(P("tok", "heads"),) * 6 + (P("heads"),) * 4,
        out_specs=(P("tok", "heads"), P("tok", "heads")),
        check_vma=False,
    )
```

```python
import functools
import heapq
import jax
import jax.numpy as jnp
from jax import lax
from jax.experimental import pallas as pl
from jax.experimental.pallas import tpu as pltpu
from jax.sharding import PartitionSpec as P

HEADS = 32
HD = 64
EPS = 1e-06
LOG2E = 1.4426950408889634
NX, NZ, NH = 4, 8, 8
NT = (((1,), (1,)), ((), ()))
BF = jnp.bfloat16
F32 = jnp.float32
MESH = pl.DeviceIdType.MESH
TQ = 256
TK = 512

SCHEME = (1, 1, 1, 0, 1, 0)
BLOCK_US, HOP_US, LATE_US, FAR_US = 0.352, 3.3, 3.5, 0.75


def plan():
    items = len(SCHEME)

    def signed(v, n):
        return v if v <= n // 2 else v - n

    def onward(key):
        t, dx, dz = key
        np_, ns = (NZ, NX) if SCHEME[t] else (NX, NZ)
        p, s = (signed(dz, NZ), signed(dx, NX)) if SCHEME[t] else (signed(dx, NX), signed(dz, NZ))
        out = []
        if s == 0:
            if p == 0:
                out += [("p", d) for d in range(np_ // 2, -((np_ + 1) // 2), -1) if d not in (0, -np_ // 2)]
            out += [("s", d) for d in ((1, -1) if ns == 4 else (2, -2, 1, -1))]
        else:
            back = -1 if s > 0 else 1
            side = (s < 0) == (p % 2 == 0)
            if abs(s) == ns // 4:
                if ns == 8:
                    out.append(("s", back))
                if side:
                    out.append(("s", back * ns // 4))
        return p, s, out

    queue, busy, events, order, count, land = {}, {}, [], [], 0, {}
    for t in range(items):
        heapq.heappush(events, (0.0 if t < 2 else LATE_US, t, 0, (t, 0, 0)))
    count = items
    while events:
        now, _, kind, x = heapq.heappop(events)
        if kind == 0:
            p, s, out = onward(x)
            cz, cx = ((1 - 2 * (s % 2)) * p, (1 - 2 * (p % 2)) * s) if SCHEME[x[0]] else ((1 - 2 * (p % 2)) * s, (1 - 2 * (s % 2)) * p)
            cz, cx = (NZ // 2 if cz == -(NZ // 2) else cz), (NX // 2 if cx == -(NX // 2) else cx)
            if x[0] < 4:
                land[cx, cz] = max(land.get((cx, cz), 0.0), now)
            for a, d in out:
                link = ("z" if (a == "p") == bool(SCHEME[x[0]]) else "x", 1 if d > 0 else -1)
                count += 2
                heapq.heappush(queue.setdefault(link, []), (int(x[0] >= 4), int(a == "s"), -abs(d), now, count, x, p, s, a, d))
                heapq.heappush(events, (max(now, busy.get(link, 0.0)), count + 1, 1, link))
        elif queue.get(x):
            if now < busy.get(x, 0.0) - 1e-9:
                count += 1
                heapq.heappush(events, (busy[x], count, 1, x))
                continue
            _, _, _, _, _, key, p, s, a, d = heapq.heappop(queue[x])
            even_p = 1 - 2 * (p % 2)
            order.append((key[0], (1 - 2 * (s % 2)) * p, even_p * s, a, d * (1 if a == "p" else even_p), now))
            both = 2 * abs(d) == (NZ if x[0] == "z" else NX)
            wire = BLOCK_US * abs(d) * (0.5 if both else 1.0)
            busy[x] = now + wire
            if both:
                busy[x[0], -x[1]] = max(busy.get((x[0], -x[1]), 0.0), now) + wire
            t, dx, dz = key
            landed = (t, dx, (dz - d) % NZ) if x[0] == "z" else (t, (dx - d) % NX, dz)
            count += 1
            heapq.heappush(events, (now + wire + HOP_US + FAR_US * (abs(d) - 1), count, 0, landed))
            count += 1
            heapq.heappush(events, (busy[x], count, 1, x))
    assert len(order) == items * (NX * NZ - 1)
    return order


def make_rhs(x, h, factor):
    x = x.astype(F32) * factor
    lane = lax.broadcasted_iota(jnp.int32, x.shape, 1)
    x = jnp.where((lane // HD) == (h % 2), x, 0.0)
    hi = x.astype(BF)
    lo = (x - hi.astype(F32)).astype(BF)
    return jnp.concatenate([hi, lo], axis=1)


def pair_of(h):
    return pl.ds(pl.multiple_of((h // 2) * 128, 128), 128)


def scores_step(k_ref, h, kt, tk, rhs, s_ref, m):
    pair = pl.multiple_of((h // 2) * 128, 128)
    kk = k_ref[pl.ds(kt * tk, tk), pl.ds(pair, 128)]
    s = lax.dot_general(jnp.concatenate([kk, kk], axis=1), rhs, NT, preferred_element_type=F32)
    s_ref[pl.ds(kt * tk, tk), :] = s
    part = jnp.max(s.reshape(tk // 8, 8, s.shape[1]), axis=0)
    return part if m is None else jnp.maximum(m, part)


def mix_step(v_ref, h, kt, tk, s_ref, m, acc):
    p = jnp.exp2(s_ref[pl.ds(kt * tk, tk), :] - m).astype(BF)
    part = jnp.dot(v_ref[h, :, pl.ds(kt * tk, tk)], p, preferred_element_type=F32)
    return part if acc is None else acc + part


class Pipe:
    def __init__(self, item, k_ref, v_ref, keys, factor, s_refs, m_refs, finish):
        self.item, self.k, self.v, self.keys, self.factor = item, k_ref, v_ref, keys, factor
        self.s, self.m, self.finish = s_refs, m_refs, finish

    def scores(self, i, now, mix=None):
        h, x = self.item(i)
        rhs = make_rhs(x, h, self.factor)
        m, acc = None, None
        for kt in range(self.keys // TK):
            m = scores_step(self.k, h, kt, TK, rhs, self.s[now], m)
            if mix is not None:
                acc = mix_step(self.v, mix[0], kt, TK, self.s[1 - now], mix[1], acc)
        self.m[now][...] = jnp.broadcast_to(jnp.max(m, axis=0, keepdims=True), (8, TQ))
        return acc

    def one(self, i, now):
        prev = self.m[1 - now][0:1]
        h = (i - 1) % 4
        acc = self.scores(i, now, (h, prev))
        self.finish(i - 1, h, acc, prev)

    def last(self, i, now):
        prev = self.m[now][0:1]
        h = i % 4
        acc = None
        for kt in range(self.keys // TK):
            acc = mix_step(self.v, h, kt, TK, self.s[now], prev, acc)
        self.finish(i, h, acc, prev)


def row_sums(x):
    x = x.astype(F32)
    y = x[:, :128] * x[:, :128] + x[:, 128:] * x[:, 128:]
    return jnp.sum(jnp.transpose(y), axis=0, keepdims=True)


def along_rows(row):
    return jnp.transpose(jnp.broadcast_to(row, (128, 128)))


def scaled(x, col, gain):
    c = jnp.concatenate([col, col], axis=1)
    return (x.astype(F32) * c * gain).astype(BF)


def kernel(vq_h, vk_h, vv_h, aq_h, ak_h, av_h, gvq_h, gak_h, gaq_h, gvk_h, vout_h, aout,
           vq, vk, vv, gains, araw, va, ka, qa, vT, voT, vvT, sa, sb, ma, mb,
           sta_own, sta_all, st_own, st_all, pT, xrecv, lse, lrecv, zsend, zrecv, lsend, lzrecv, vout,
           in_sem, out_sem, sta_send, sta_recv, st_send, st_recv, g_send, g_recv, x_send, x_recv, xl_send, xl_recv, z_send, z_recv, zl_send, zl_recv):
    hx = lax.axis_index("heads")
    tok = lax.axis_index("tok")
    x0, z0 = tok // NZ, tok % NZ
    n, na, ar = vq.shape[0], ka.shape[0], araw.shape[1]

    def at(x, z):
        return (x % NX) * NZ + (z % NZ)

    ins = [pltpu.make_async_copy(vq_h, vq, in_sem.at[0]), pltpu.make_async_copy(vk_h, vk, in_sem.at[1]),
           pltpu.make_async_copy(aq_h, araw.at[1], in_sem.at[2]), pltpu.make_async_copy(ak_h, araw.at[0], in_sem.at[3]),
           pltpu.make_async_copy(av_h, va.at[pl.ds(pl.multiple_of(tok * ar, ar), ar)], in_sem.at[4]),
           pltpu.make_async_copy(vv_h, vv, in_sem.at[5])]
    ins += [pltpu.make_async_copy(g, gains.at[i], in_sem.at[6 + i]) for i, g in enumerate((gvq_h, gak_h, gaq_h, gvk_h))]
    for i in (2, 3, 4, 0, 1, 6, 7, 8, 9, 5):
        ins[i].start()

    peers = [{"heads": (hx + i) % NH} for i in range(1, NH)]
    peers += [{"tok": at(x0 + i, z0)} for i in range(1, NX)] + [{"tok": at(x0, z0 + i)} for i in range(1, NZ)]
    barrier = pltpu.get_barrier_semaphore()
    for p in peers:
        pl.semaphore_signal(barrier, inc=1, device_id=p, device_id_type=MESH)
    sta_own[...] = jnp.zeros_like(sta_own)
    ins[2].wait()
    ins[3].wait()
    sta_own[0:1, :] = row_sums(araw[...].reshape(2 * ar, 256))
    ins[4].wait()
    pl.semaphore_wait(barrier, len(peers))

    half = ar // 2
    bufs = (va, va, ka, ka, qa, qa)
    odd_x, odd_z = 1 - 2 * (x0 % 2), 1 - 2 * (z0 % 2)
    order = plan()
    waited = {(t, 0, 0) for t in range(6)}

    def source(t, p, s):
        zf = SCHEME[t]
        sp = (odd_x if zf else odd_z) * (1 - 2 * (s % 2))
        ss = (odd_z if zf else odd_x) * (1 - 2 * (p % 2))
        po, so = sp * p, ss * s
        return at(x0 + so, z0 + po) if zf else at(x0 + po, z0 + so)

    def piece(t, b):
        return bufs[t].at[pl.ds(pl.multiple_of(b * ar + (t % 2) * half, half), half)]

    def arrived(t, p, s):
        np_, ns = (NZ, NX) if SCHEME[t] else (NX, NZ)
        if p == -(np_ // 2):
            p = np_ // 2
        if s == -(ns // 2):
            s = ns // 2
        if (t, p, s) not in waited:
            waited.add((t, p, s))
            b = source(t, p, s)
            ref = piece(t, b)
            pltpu.make_async_copy(ref, ref, g_recv.at[t, b]).wait()

    done = [0]

    def pump(until=None, upto=None):
        while done[0] < len(order):
            t, p, s, a, d, when = order[done[0]]
            if (until is not None and when > until) or (upto is not None and done[0] >= upto):
                return
            arrived(t, p, s)
            zf = SCHEME[t]
            sign = (odd_x if zf else odd_z) if a == "p" else (odd_z if zf else odd_x) * (1 - 2 * (p % 2))
            step = sign * d
            to = at(x0, z0 + step) if (a == "p") == bool(zf) else at(x0 + step, z0)
            b = source(t, p, s)
            ref = piece(t, b)
            pltpu.make_async_remote_copy(src_ref=ref, dst_ref=ref, send_sem=g_send.at[t], recv_sem=g_recv.at[t, b],
                                         device_id={"tok": to}, device_id_type=MESH).start()
            done[0] += 1

    def complete(ts):
        for t in ts:
            np_, ns = (NZ, NX) if SCHEME[t] else (NX, NZ)
            for p in range(1 - np_ // 2, np_ // 2 + 1):
                for s in range(1 - ns // 2, ns // 2 + 1):
                    arrived(t, p, s)

    def to_heads(own, every, send, recv):
        out = []
        for i in range(1, NH):
            c = pltpu.make_async_remote_copy(src_ref=own, dst_ref=every.at[i - 1], send_sem=send.at[i - 1], recv_sem=recv.at[i - 1],
                                             device_id={"heads": (hx + i) % NH}, device_id_type=MESH)
            c.start()
            out.append(c)
        return out

    def scale_of(copies, own, every):
        for c in copies:
            c.wait()
        total = own[...]
        for i in range(NH - 1):
            total = total + every[i]
        return lax.rsqrt(total * (1.0 / (HEADS * HD)) + EPS)

    a_copies = to_heads(sta_own, sta_all, sta_send, sta_recv)
    pump(until=0.1)
    for i, ref in ((0, vq), (1, vk)):
        ins[i].wait()
        for c in range(n // 128):
            st_own[i * 8 + c:i * 8 + c + 1, :] = row_sums(ref[c * 128:(c + 1) * 128, :])
    v_copies = to_heads(st_own, st_all, st_send, st_recv)
    for i in range(6, 10):
        ins[i].wait()
    col = along_rows(scale_of(a_copies, sta_own, sta_all)[0:1])
    mine = pl.ds(pl.multiple_of(tok * ar, ar), ar)
    ka[mine, :] = scaled(araw[0], col[0:ar], gains[1])
    qa[mine, :] = scaled(araw[1], col[ar:2 * ar], gains[2])
    pump(until=LATE_US + 0.4)
    ins[5].wait()
    for c in range(0, n, 256):
        t = jnp.transpose(vv[c:c + 256, :])
        for h in range(4):
            vvT[h, :, c:c + 256] = t[h * HD:(h + 1) * HD]
            voT[h, HD:HD + 16, c:c + 256] = jnp.ones((16, 256), BF)
    pump(until=LATE_US + 1.0)
    scale = scale_of(v_copies, st_own, st_all)
    factor = HD ** (-0.5) * LOG2E
    for qt in range(n // TQ):
        for c in range(qt * TQ // 128, (qt + 1) * TQ // 128):
            vq[c * 128:(c + 1) * 128, :] = scaled(vq[c * 128:(c + 1) * 128, :], along_rows(scale[c:c + 1]), gains[0])
        pump(until=LATE_US + 1.6 + 0.6 * qt)
    for c in range(n // 128):
        vk[c * 128:(c + 1) * 128, :] = scaled(vk[c * 128:(c + 1) * 128, :], along_rows(scale[8 + c:9 + c]), gains[3])

    pump(upto=1 + max(i for i, o in enumerate(order) if o[0] < 4))
    complete((0, 1))
    for c in range(0, na, 256):
        t = jnp.transpose(va[c:c + 256, :])
        for h in range(4):
            vT[h, 0:HD, c:c + 256] = t[h * HD:(h + 1) * HD]
            vT[h, HD:HD + 16, c:c + 256] = jnp.ones((16, 256), BF)
    complete((2, 3))

    def item1(i):
        return i % 4, vq[(i // 4) * TQ:(i // 4 + 1) * TQ, (i % 4 // 2) * 128:(i % 4 // 2 + 1) * 128]

    def finish1(i, h, acc, m):
        r0 = (i // 4) * TQ
        o = acc[0:HD] * (1.0 / acc[HD:HD + 1])
        voT[h, 0:HD, r0:r0 + TQ] = (vvT[h, :, r0:r0 + TQ].astype(F32) + o).astype(BF)

    one = Pipe(item1, ka, vT, na, factor, (sa, sb), (ma, mb), finish1)
    n1 = 4 * (n // TQ)
    left = len(order) - done[0]
    start = done[0]
    one.scores(0, 0)
    for i in range(1, n1):
        pump(upto=start + (left * i) // (n1 - 4))
        one.one(i, i % 2)
    one.last(n1 - 1, (n1 - 1) % 2)
    pump()
    complete((4, 5))

    slab = na // NX

    def slab_of(k):
        o = jnp.where(k == 0, 2, jnp.where(k == 1, 1, jnp.where(k == 2, 3, 0)))
        return (x0 + o) % NX

    def item2(i):
        h, k, hh = i % 4, (i // 4) % 4, i // 16
        base = slab_of(k) * slab + hh * ar
        x = [qa[pl.ds(pl.multiple_of(base + 2 * j * ar, ar), ar), pair_of(h)] for j in range(4)]
        return h, jnp.concatenate(x, axis=0)

    def finish2(i, h, acc, m):
        p = i // 4
        o = acc[0:HD] * (1.0 / acc[HD:HD + 1])
        pT[p, pl.ds(pl.multiple_of(h * HD, HD), HD), :] = o.astype(BF)
        lse[p, pl.ds(h, 1), :] = m + jnp.log2(acc[HD:HD + 1])

    def x_pair(p, k, to):
        a = pltpu.make_async_remote_copy(src_ref=pT.at[p], dst_ref=xrecv.at[p], send_sem=x_send.at[p], recv_sem=x_recv.at[p],
                                         device_id={"tok": at(to, z0)}, device_id_type=MESH)
        b = pltpu.make_async_remote_copy(src_ref=lse.at[p], dst_ref=lrecv.at[p], send_sem=xl_send.at[p], recv_sem=xl_recv.at[p],
                                         device_id={"tok": at(to, z0)}, device_id_type=MESH)
        return a, b

    two = Pipe(item2, vk, voT, n, factor, (sa, sb), (ma, mb), finish2)
    two.scores(0, 0)

    def trip(p, c):
        for j in range(4):
            two.one(4 * p + j + 1, (j + 1) % 2)

        @pl.when(p % 4 < 3)
        def _():
            for c_ in x_pair(p, p % 4, slab_of(p % 4)):
                c_.start()

        return c

    lax.fori_loop(0, 7, trip, 0)
    for j in range(3):
        two.one(29 + j, (j + 1) % 2)
    two.last(31, 1)

    for c in range(0, n, 256):
        t = jnp.concatenate([voT[h, 0:HD, c:c + 256] for h in range(4)], axis=0)
        vout[c:c + 256, :] = jnp.transpose(t)
    out_copy = pltpu.make_async_copy(vout, vout_h, out_sem)
    out_copy.start()

    def z_pair(i):
        zt = (z0 + i) % NZ
        hh, j = zt % 2, zt // 2
        a = pltpu.make_async_remote_copy(src_ref=zsend.at[hh, pl.ds(pl.multiple_of(j * ar, ar), ar)], dst_ref=zrecv.at[i - 1],
                                         send_sem=z_send.at[i - 1], recv_sem=z_recv.at[i - 1], device_id={"tok": at(x0, zt)}, device_id_type=MESH)
        b = pltpu.make_async_remote_copy(src_ref=lsend.at[hh, :, pl.ds(pl.multiple_of((j // 2) * 128, 128), 128)], dst_ref=lzrecv.at[i - 1],
                                         send_sem=zl_send.at[i - 1], recv_sem=zl_recv.at[i - 1], device_id={"tok": at(x0, zt)}, device_id_type=MESH)
        return a, b

    for hh in range(2):
        for k in range(3):
            for c in x_pair(hh * 4 + k, k, slab_of(k)):
                c.wait()
        ls = [lrecv[hh * 4 + k] for k in range(3)] + [lse[hh * 4 + 3]]
        top = functools.reduce(jnp.maximum, [l[0:4] for l in ls])
        ws = [jnp.exp2(l[0:4] - top) for l in ls]
        tot = ws[0] + ws[1] + ws[2] + ws[3]
        inv = 1.0 / tot
        lsend[hh, 0:4, :] = top + jnp.log2(tot)
        lsend[hh, 4:8, :] = jnp.zeros((4, TQ), F32)
        ws = [w * inv for w in ws]
        parts = []
        for h in range(4):
            o = pT[hh * 4 + 3, h * HD:(h + 1) * HD, :].astype(F32) * ws[3][h:h + 1]
            for k in range(3):
                o = o + xrecv[hh * 4 + k, h * HD:(h + 1) * HD, :].astype(F32) * ws[k][h:h + 1]
            parts.append(o.astype(BF))
        zsend[hh] = jnp.transpose(jnp.concatenate(parts, axis=0))
        for j in range(4):
            i = 2 * j + 2 - (z0 + hh) % 2

            @pl.when(i < NZ)
            def _():
                for c in z_pair(i):
                    c.start()

    for i in range(1, NZ):
        for c in z_pair(i):
            c.wait()
    own = z0 % 2
    ls = [lzrecv[i] for i in range(NZ - 1)] + [lsend[own, :, pl.ds(pl.multiple_of((z0 // 4) * 128, 128), 128)]]
    top = functools.reduce(jnp.maximum, ls)
    ws = [jnp.exp2(l - top) for l in ls]
    inv = 1.0 / functools.reduce(jnp.add, ws)
    odd = ((z0 // 2) % 2) == 1
    acc = jnp.zeros((ar, 256), F32)
    for i in range(NZ):
        w = ws[i] * inv
        cols = []
        for h in range(4):
            t = jnp.transpose(jnp.broadcast_to(w[h:h + 1], (128, 128)))
            cols.append(jnp.where(odd, t[ar:2 * ar, 0:HD], t[0:ar, 0:HD]))
        wide = jnp.concatenate(cols, axis=1)
        o = zrecv[i] if i < NZ - 1 else zsend[own, pl.ds(pl.multiple_of((z0 // 2) * ar, ar), ar), :]
        acc = acc + o.astype(F32) * wide
    aout[...] = acc.astype(BF)
    for t in range(6):
        rows = bufs[t].at[pl.ds(0, (NX * NZ - 1) * half)]
        pltpu.make_async_copy(rows, rows, g_send.at[t]).wait()
    out_copy.wait()


def body(video_q, video_k, video_v, audio_q, audio_k, audio_v, video_q_gain, audio_k_gain, audio_q_gain, video_k_gain):
    n, w = video_q.shape
    ar = audio_q.shape[0]
    na = ar * NX * NZ
    A = pl.BlockSpec(memory_space=pl.ANY)
    V = pl.BlockSpec(memory_space=pltpu.VMEM)
    M = pltpu.VMEM
    D = pltpu.SemaphoreType.DMA
    return pl.pallas_call(
        kernel,
        out_shape=(jax.ShapeDtypeStruct((n, w), BF), jax.ShapeDtypeStruct((ar, w), BF)),
        in_specs=[A] * 10,
        out_specs=(A, V),
        scratch_shapes=[
            M((n, w), BF), M((n, w), BF), M((n, w), BF), M((4, 1, w), F32), M((2, ar, w), BF), M((na, w), BF), M((na, w), BF), M((na, w), BF),
            M((4, HD + 16, na), BF), M((4, HD + 16, n), BF), M((4, HD, n), BF),
            M((na, TQ), F32), M((na, TQ), F32), M((8, TQ), F32), M((8, TQ), F32),
            M((8, 128), F32), M((NH - 1, 8, 128), F32), M((16, 128), F32), M((NH - 1, 16, 128), F32),
            M((8, w, TQ), BF), M((8, w, TQ), BF), M((8, 8, TQ), F32), M((8, 8, TQ), F32),
            M((2, TQ, w), BF), M((NZ - 1, ar, w), BF), M((2, 8, TQ), F32), M((NZ - 1, 8, 128), F32), M((n, w), BF),
            D((10,)), D, D((NH - 1,)), D((NH - 1,)), D((NH - 1,)), D((NH - 1,)), D((6,)), D((6, NX * NZ)),
            D((8,)), D((8,)), D((8,)), D((8,)), D((NZ - 1,)), D((NZ - 1,)), D((NZ - 1,)), D((NZ - 1,)),
        ],
        compiler_params=pltpu.CompilerParams(collective_id=0, has_side_effects=True, vmem_limit_bytes=60 * 2**20),
        name="av_cross",
    )(video_q, video_k, video_v, audio_q, audio_k, audio_v, video_q_gain[None], audio_k_gain[None], audio_q_gain[None], video_k_gain[None])


def solution(mesh):
    return jax.shard_map(
        body,
        mesh=mesh,
        in_specs=(P("tok", "heads"),) * 6 + (P("heads"),) * 4,
        out_specs=(P("tok", "heads"), P("tok", "heads")),
        check_vma=False,
    )
```

```python
import functools
import heapq
import jax
import jax.numpy as jnp
from jax import lax
from jax.experimental import pallas as pl
from jax.experimental.pallas import tpu as pltpu
from jax.sharding import PartitionSpec as P

HEADS = 32
HD = 64
EPS = 1e-06
LOG2E = 1.4426950408889634
NX, NZ, NH = 4, 8, 8
NT = (((1,), (1,)), ((), ()))
BF = jnp.bfloat16
F32 = jnp.float32
MESH = pl.DeviceIdType.MESH
TQ = 256
TK = 512

SCHEME = (1, 1, 1, 0, 1, 0)
BLOCK_US, HOP_US, LATE_US, FAR_US = 0.352, 3.3, 3.5, 0.75


def plan():
    items = len(SCHEME)

    def signed(v, n):
        return v if v <= n // 2 else v - n

    def onward(key):
        t, dx, dz = key
        np_, ns = (NZ, NX) if SCHEME[t] else (NX, NZ)
        p, s = (signed(dz, NZ), signed(dx, NX)) if SCHEME[t] else (signed(dx, NX), signed(dz, NZ))
        out = []
        if s == 0:
            if p == 0:
                out += [("p", d) for d in range(np_ // 2, -((np_ + 1) // 2), -1) if d not in (0, -np_ // 2)]
            out += [("s", d) for d in ((1, -1) if ns == 4 else (2, -2, 1, -1))]
        else:
            back = -1 if s > 0 else 1
            side = (s < 0) == (p % 2 == 0)
            if abs(s) == ns // 4:
                if ns == 8:
                    out.append(("s", back))
                if side:
                    out.append(("s", back * ns // 4))
        return p, s, out

    queue, busy, events, order, count, land = {}, {}, [], [], 0, {}
    for t in range(items):
        heapq.heappush(events, (0.0 if t < 2 else LATE_US, t, 0, (t, 0, 0)))
    count = items
    while events:
        now, _, kind, x = heapq.heappop(events)
        if kind == 0:
            p, s, out = onward(x)
            cz, cx = ((1 - 2 * (s % 2)) * p, (1 - 2 * (p % 2)) * s) if SCHEME[x[0]] else ((1 - 2 * (p % 2)) * s, (1 - 2 * (s % 2)) * p)
            cz, cx = (NZ // 2 if cz == -(NZ // 2) else cz), (NX // 2 if cx == -(NX // 2) else cx)
            if x[0] < 4:
                land[cx, cz] = max(land.get((cx, cz), 0.0), now)
            for a, d in out:
                link = ("z" if (a == "p") == bool(SCHEME[x[0]]) else "x", 1 if d > 0 else -1)
                count += 2
                heapq.heappush(queue.setdefault(link, []), (int(x[0] >= 4), int(a == "s"), -abs(d), now, count, x, p, s, a, d))
                heapq.heappush(events, (max(now, busy.get(link, 0.0)), count + 1, 1, link))
        elif queue.get(x):
            if now < busy.get(x, 0.0) - 1e-9:
                count += 1
                heapq.heappush(events, (busy[x], count, 1, x))
                continue
            _, _, _, _, _, key, p, s, a, d = heapq.heappop(queue[x])
            even_p = 1 - 2 * (p % 2)
            order.append((key[0], (1 - 2 * (s % 2)) * p, even_p * s, a, d * (1 if a == "p" else even_p), now))
            both = 2 * abs(d) == (NZ if x[0] == "z" else NX)
            wire = BLOCK_US * abs(d) * (0.5 if both else 1.0)
            busy[x] = now + wire
            if both:
                busy[x[0], -x[1]] = max(busy.get((x[0], -x[1]), 0.0), now) + wire
            t, dx, dz = key
            landed = (t, dx, (dz - d) % NZ) if x[0] == "z" else (t, (dx - d) % NX, dz)
            count += 1
            heapq.heappush(events, (now + wire + HOP_US + FAR_US * (abs(d) - 1), count, 0, landed))
            count += 1
            heapq.heappush(events, (busy[x], count, 1, x))
    assert len(order) == items * (NX * NZ - 1)
    return order


def make_rhs(x, h, factor):
    x = x.astype(F32) * factor
    lane = lax.broadcasted_iota(jnp.int32, x.shape, 1)
    x = jnp.where((lane // HD) == (h % 2), x, 0.0)
    hi = x.astype(BF)
    lo = (x - hi.astype(F32)).astype(BF)
    return jnp.concatenate([hi, lo], axis=1)


def pair_of(h):
    return pl.ds(pl.multiple_of((h // 2) * 128, 128), 128)


def scores_step(k_ref, h, kt, tk, rhs, s_ref, m):
    pair = pl.multiple_of((h // 2) * 128, 128)
    kk = k_ref[pl.ds(kt * tk, tk), pl.ds(pair, 128)]
    s = lax.dot_general(jnp.concatenate([kk, kk], axis=1), rhs, NT, preferred_element_type=F32)
    s_ref[pl.ds(kt * tk, tk), :] = s
    part = jnp.max(s.reshape(tk // 8, 8, s.shape[1]), axis=0)
    return part if m is None else jnp.maximum(m, part)


def mix_step(v_ref, h, kt, tk, s_ref, m, acc):
    p = jnp.exp2(s_ref[pl.ds(kt * tk, tk), :] - m).astype(BF)
    part = jnp.dot(v_ref[h, :, pl.ds(kt * tk, tk)], p, preferred_element_type=F32)
    return part if acc is None else acc + part


class Pipe:
    def __init__(self, item, k_ref, v_ref, keys, factor, s_refs, m_refs, finish):
        self.item, self.k, self.v, self.keys, self.factor = item, k_ref, v_ref, keys, factor
        self.s, self.m, self.finish = s_refs, m_refs, finish

    def scores(self, i, now, mix=None):
        h, x = self.item(i)
        rhs = make_rhs(x, h, self.factor)
        m, acc = None, None
        for kt in range(self.keys // TK):
            m = scores_step(self.k, h, kt, TK, rhs, self.s[now], m)
            if mix is not None:
                acc = mix_step(self.v, mix[0], kt, TK, self.s[1 - now], mix[1], acc)
        self.m[now][...] = jnp.broadcast_to(jnp.max(m, axis=0, keepdims=True), (8, TQ))
        return acc

    def one(self, i, now):
        prev = self.m[1 - now][0:1]
        h = (i - 1) % 4
        acc = self.scores(i, now, (h, prev))
        self.finish(i - 1, h, acc, prev)

    def last(self, i, now):
        prev = self.m[now][0:1]
        h = i % 4
        acc = None
        for kt in range(self.keys // TK):
            acc = mix_step(self.v, h, kt, TK, self.s[now], prev, acc)
        self.finish(i, h, acc, prev)


def row_sums(x):
    x = x.astype(F32)
    y = x[:, :128] * x[:, :128] + x[:, 128:] * x[:, 128:]
    return jnp.sum(jnp.transpose(y), axis=0, keepdims=True)


def along_rows(row):
    return jnp.transpose(jnp.broadcast_to(row, (128, 128)))


def scaled(x, col, gain):
    c = jnp.concatenate([col, col], axis=1)
    return (x.astype(F32) * c * gain).astype(BF)


def kernel(vq_h, vk_h, vv_h, aq_h, ak_h, av_h, gvq_h, gak_h, gaq_h, gvk_h, vout_h, aout,
           vq, vk, vv, gains, araw, va, ka, qa, vT, voT, vvT, sa, sb, ma, mb,
           sta_own, sta_all, st_own, st_all, pT, xrecv, lse, lrecv, zsend, zrecv, lsend, lzrecv, vout,
           in_sem, out_sem, sta_send, sta_recv, st_send, st_recv, g_send, g_recv, x_send, x_recv, xl_send, xl_recv, z_send, z_recv, zl_send, zl_recv):
    hx = lax.axis_index("heads")
    tok = lax.axis_index("tok")
    x0, z0 = tok // NZ, tok % NZ
    n, na, ar = vq.shape[0], ka.shape[0], araw.shape[1]

    def at(x, z):
        return (x % NX) * NZ + (z % NZ)

    ins = [pltpu.make_async_copy(vq_h, vq, in_sem.at[0]), pltpu.make_async_copy(vk_h, vk, in_sem.at[1]),
           pltpu.make_async_copy(aq_h, araw.at[1], in_sem.at[2]), pltpu.make_async_copy(ak_h, araw.at[0], in_sem.at[3]),
           pltpu.make_async_copy(av_h, va.at[pl.ds(pl.multiple_of(tok * ar, ar), ar)], in_sem.at[4]),
           pltpu.make_async_copy(vv_h, vv, in_sem.at[5])]
    ins += [pltpu.make_async_copy(g, gains.at[i], in_sem.at[6 + i]) for i, g in enumerate((gvq_h, gak_h, gaq_h, gvk_h))]
    for i in (2, 3, 4, 0, 1, 6, 7, 8, 9, 5):
        ins[i].start()

    peers = [{"heads": (hx + i) % NH} for i in range(1, NH)]
    peers += [{"tok": at(x0 + i, z0)} for i in range(1, NX)] + [{"tok": at(x0, z0 + i)} for i in range(1, NZ)]
    barrier = pltpu.get_barrier_semaphore()
    for p in peers:
        pl.semaphore_signal(barrier, inc=1, device_id=p, device_id_type=MESH)
    sta_own[...] = jnp.zeros_like(sta_own)
    ins[2].wait()
    ins[3].wait()
    sta_own[0:1, :] = row_sums(araw[...].reshape(2 * ar, 256))
    ins[4].wait()
    pl.semaphore_wait(barrier, len(peers))

    half = ar // 2
    bufs = (va, va, ka, ka, qa, qa)
    odd_x, odd_z = 1 - 2 * (x0 % 2), 1 - 2 * (z0 % 2)
    order = plan()
    waited = {(t, 0, 0) for t in range(6)}

    def source(t, p, s):
        zf = SCHEME[t]
        sp = (odd_x if zf else odd_z) * (1 - 2 * (s % 2))
        ss = (odd_z if zf else odd_x) * (1 - 2 * (p % 2))
        po, so = sp * p, ss * s
        return at(x0 + so, z0 + po) if zf else at(x0 + po, z0 + so)

    def piece(t, b):
        return bufs[t].at[pl.ds(pl.multiple_of(b * ar + (t % 2) * half, half), half)]

    def arrived(t, p, s):
        np_, ns = (NZ, NX) if SCHEME[t] else (NX, NZ)
        if p == -(np_ // 2):
            p = np_ // 2
        if s == -(ns // 2):
            s = ns // 2
        if (t, p, s) not in waited:
            waited.add((t, p, s))
            b = source(t, p, s)
            ref = piece(t, b)
            pltpu.make_async_copy(ref, ref, g_recv.at[t, b]).wait()

    done = [0]

    def pump(until=None, upto=None):
        while done[0] < len(order):
            t, p, s, a, d, when = order[done[0]]
            if (until is not None and when > until) or (upto is not None and done[0] >= upto):
                return
            arrived(t, p, s)
            zf = SCHEME[t]
            sign = (odd_x if zf else odd_z) if a == "p" else (odd_z if zf else odd_x) * (1 - 2 * (p % 2))
            step = sign * d
            to = at(x0, z0 + step) if (a == "p") == bool(zf) else at(x0 + step, z0)
            b = source(t, p, s)
            ref = piece(t, b)
            pltpu.make_async_remote_copy(src_ref=ref, dst_ref=ref, send_sem=g_send.at[t], recv_sem=g_recv.at[t, b],
                                         device_id={"tok": to}, device_id_type=MESH).start()
            done[0] += 1

    def complete(ts):
        for t in ts:
            np_, ns = (NZ, NX) if SCHEME[t] else (NX, NZ)
            for p in range(1 - np_ // 2, np_ // 2 + 1):
                for s in range(1 - ns // 2, ns // 2 + 1):
                    arrived(t, p, s)

    def to_heads(own, every, send, recv):
        out = []
        for i in range(1, NH):
            c = pltpu.make_async_remote_copy(src_ref=own, dst_ref=every.at[i - 1], send_sem=send.at[i - 1], recv_sem=recv.at[i - 1],
                                             device_id={"heads": (hx + i) % NH}, device_id_type=MESH)
            c.start()
            out.append(c)
        return out

    def scale_of(copies, own, every):
        for c in copies:
            c.wait()
        total = own[...]
        for i in range(NH - 1):
            total = total + every[i]
        return lax.rsqrt(total * (1.0 / (HEADS * HD)) + EPS)

    a_copies = to_heads(sta_own, sta_all, sta_send, sta_recv)
    pump(until=0.1)
    for i, ref in ((0, vq), (1, vk)):
        ins[i].wait()
        for c in range(n // 128):
            st_own[i * 8 + c:i * 8 + c + 1, :] = row_sums(ref[c * 128:(c + 1) * 128, :])
    v_copies = to_heads(st_own, st_all, st_send, st_recv)
    for i in range(6, 10):
        ins[i].wait()
    col = along_rows(scale_of(a_copies, sta_own, sta_all)[0:1])
    mine = pl.ds(pl.multiple_of(tok * ar, ar), ar)
    ka[mine, :] = scaled(araw[0], col[0:ar], gains[1])
    qa[mine, :] = scaled(araw[1], col[ar:2 * ar], gains[2])
    pump(until=LATE_US + 0.4)
    ins[5].wait()
    for c in range(0, n, 256):
        t = jnp.transpose(vv[c:c + 256, :])
        for h in range(4):
            vvT[h, :, c:c + 256] = t[h * HD:(h + 1) * HD]
            voT[h, HD:HD + 16, c:c + 256] = jnp.ones((16, 256), BF)
    pump(until=LATE_US + 1.0)
    scale = scale_of(v_copies, st_own, st_all)
    factor = HD ** (-0.5) * LOG2E
    for qt in range(n // TQ):
        for c in range(qt * TQ // 128, (qt + 1) * TQ // 128):
            vq[c * 128:(c + 1) * 128, :] = scaled(vq[c * 128:(c + 1) * 128, :], along_rows(scale[c:c + 1]), gains[0])
        pump(until=LATE_US + 1.6 + 0.6 * qt)
    for c in range(n // 128):
        vk[c * 128:(c + 1) * 128, :] = scaled(vk[c * 128:(c + 1) * 128, :], along_rows(scale[8 + c:9 + c]), gains[3])

    pump(upto=1 + max(i for i, o in enumerate(order) if o[0] < 4))
    complete((0, 1))
    for c in range(0, na, 256):
        t = jnp.transpose(va[c:c + 256, :])
        for h in range(4):
            vT[h, 0:HD, c:c + 256] = t[h * HD:(h + 1) * HD]
            vT[h, HD:HD + 16, c:c + 256] = jnp.ones((16, 256), BF)
    complete((2, 3))

    def item1(i):
        return i % 4, vq[(i // 4) * TQ:(i // 4 + 1) * TQ, (i % 4 // 2) * 128:(i % 4 // 2 + 1) * 128]

    def finish1(i, h, acc, m):
        r0 = (i // 4) * TQ
        o = acc[0:HD] * (1.0 / acc[HD:HD + 1])
        voT[h, 0:HD, r0:r0 + TQ] = (vvT[h, :, r0:r0 + TQ].astype(F32) + o).astype(BF)

    one = Pipe(item1, ka, vT, na, factor, (sa, sb), (ma, mb), finish1)
    n1 = 4 * (n // TQ)
    left = len(order) - done[0]
    start = done[0]
    one.scores(0, 0)
    for i in range(1, n1):
        pump(upto=start + (left * i) // (n1 - 6))
        one.one(i, i % 2)
    one.last(n1 - 1, (n1 - 1) % 2)
    pump()
    complete((4, 5))

    slab = na // NX

    def slab_of(k):
        o = jnp.where(k == 0, 2, jnp.where(k == 1, 1, jnp.where(k == 2, 3, 0)))
        return (x0 + o) % NX

    def item2(i):
        h, k, hh = i % 4, (i // 4) % 4, i // 16
        base = slab_of(k) * slab + hh * ar
        x = [qa[pl.ds(pl.multiple_of(base + 2 * j * ar, ar), ar), pair_of(h)] for j in range(4)]
        return h, jnp.concatenate(x, axis=0)

    def finish2(i, h, acc, m):
        p = i // 4
        o = acc[0:HD] * (1.0 / acc[HD:HD + 1])
        pT[p, pl.ds(pl.multiple_of(h * HD, HD), HD), :] = o.astype(BF)
        lse[p, pl.ds(h, 1), :] = m + jnp.log2(acc[HD:HD + 1])

    def x_pair(p, k, to):
        a = pltpu.make_async_remote_copy(src_ref=pT.at[p], dst_ref=xrecv.at[p], send_sem=x_send.at[p], recv_sem=x_recv.at[p],
                                         device_id={"tok": at(to, z0)}, device_id_type=MESH)
        b = pltpu.make_async_remote_copy(src_ref=lse.at[p], dst_ref=lrecv.at[p], send_sem=xl_send.at[p], recv_sem=xl_recv.at[p],
                                         device_id={"tok": at(to, z0)}, device_id_type=MESH)
        return a, b

    two = Pipe(item2, vk, voT, n, factor, (sa, sb), (ma, mb), finish2)
    two.scores(0, 0)

    def trip(p, c):
        for j in range(4):
            two.one(4 * p + j + 1, (j + 1) % 2)

        @pl.when(p % 4 < 3)
        def _():
            for c_ in x_pair(p, p % 4, slab_of(p % 4)):
                c_.start()

        return c

    lax.fori_loop(0, 7, trip, 0)
    for j in range(3):
        two.one(29 + j, (j + 1) % 2)
    two.last(31, 1)

    for c in range(0, n, 256):
        t = jnp.concatenate([voT[h, 0:HD, c:c + 256] for h in range(4)], axis=0)
        vout[c:c + 256, :] = jnp.transpose(t)
    out_copy = pltpu.make_async_copy(vout, vout_h, out_sem)
    out_copy.start()

    def z_pair(i):
        zt = (z0 + i) % NZ
        hh, j = zt % 2, zt // 2
        a = pltpu.make_async_remote_copy(src_ref=zsend.at[hh, pl.ds(pl.multiple_of(j * ar, ar), ar)], dst_ref=zrecv.at[i - 1],
                                         send_sem=z_send.at[i - 1], recv_sem=z_recv.at[i - 1], device_id={"tok": at(x0, zt)}, device_id_type=MESH)
        b = pltpu.make_async_remote_copy(src_ref=lsend.at[hh, :, pl.ds(pl.multiple_of((j // 2) * 128, 128), 128)], dst_ref=lzrecv.at[i - 1],
                                         send_sem=zl_send.at[i - 1], recv_sem=zl_recv.at[i - 1], device_id={"tok": at(x0, zt)}, device_id_type=MESH)
        return a, b

    for hh in range(2):
        for k in range(3):
            for c in x_pair(hh * 4 + k, k, slab_of(k)):
                c.wait()
        ls = [lrecv[hh * 4 + k] for k in range(3)] + [lse[hh * 4 + 3]]
        top = functools.reduce(jnp.maximum, [l[0:4] for l in ls])
        ws = [jnp.exp2(l[0:4] - top) for l in ls]
        tot = ws[0] + ws[1] + ws[2] + ws[3]
        inv = 1.0 / tot
        lsend[hh, 0:4, :] = top + jnp.log2(tot)
        lsend[hh, 4:8, :] = jnp.zeros((4, TQ), F32)
        ws = [w * inv for w in ws]
        parts = []
        for h in range(4):
            o = pT[hh * 4 + 3, h * HD:(h + 1) * HD, :].astype(F32) * ws[3][h:h + 1]
            for k in range(3):
                o = o + xrecv[hh * 4 + k, h * HD:(h + 1) * HD, :].astype(F32) * ws[k][h:h + 1]
            parts.append(o.astype(BF))
        zsend[hh] = jnp.transpose(jnp.concatenate(parts, axis=0))
        for j in range(4):
            i = 2 * j + 2 - (z0 + hh) % 2

            @pl.when(i < NZ)
            def _():
                for c in z_pair(i):
                    c.start()

    for i in range(1, NZ):
        for c in z_pair(i):
            c.wait()
    own = z0 % 2
    ls = [lzrecv[i] for i in range(NZ - 1)] + [lsend[own, :, pl.ds(pl.multiple_of((z0 // 4) * 128, 128), 128)]]
    top = functools.reduce(jnp.maximum, ls)
    ws = [jnp.exp2(l - top) for l in ls]
    inv = 1.0 / functools.reduce(jnp.add, ws)
    odd = ((z0 // 2) % 2) == 1
    acc = jnp.zeros((ar, 256), F32)
    for i in range(NZ):
        w = ws[i] * inv
        cols = []
        for h in range(4):
            t = jnp.transpose(jnp.broadcast_to(w[h:h + 1], (128, 128)))
            cols.append(jnp.where(odd, t[ar:2 * ar, 0:HD], t[0:ar, 0:HD]))
        wide = jnp.concatenate(cols, axis=1)
        o = zrecv[i] if i < NZ - 1 else zsend[own, pl.ds(pl.multiple_of((z0 // 2) * ar, ar), ar), :]
        acc = acc + o.astype(F32) * wide
    aout[...] = acc.astype(BF)
    for t in range(6):
        rows = bufs[t].at[pl.ds(0, (NX * NZ - 1) * half)]
        pltpu.make_async_copy(rows, rows, g_send.at[t]).wait()
    out_copy.wait()


def body(video_q, video_k, video_v, audio_q, audio_k, audio_v, video_q_gain, audio_k_gain, audio_q_gain, video_k_gain):
    n, w = video_q.shape
    ar = audio_q.shape[0]
    na = ar * NX * NZ
    A = pl.BlockSpec(memory_space=pl.ANY)
    V = pl.BlockSpec(memory_space=pltpu.VMEM)
    M = pltpu.VMEM
    D = pltpu.SemaphoreType.DMA
    return pl.pallas_call(
        kernel,
        out_shape=(jax.ShapeDtypeStruct((n, w), BF), jax.ShapeDtypeStruct((ar, w), BF)),
        in_specs=[A] * 10,
        out_specs=(A, V),
        scratch_shapes=[
            M((n, w), BF), M((n, w), BF), M((n, w), BF), M((4, 1, w), F32), M((2, ar, w), BF), M((na, w), BF), M((na, w), BF), M((na, w), BF),
            M((4, HD + 16, na), BF), M((4, HD + 16, n), BF), M((4, HD, n), BF),
            M((na, TQ), F32), M((na, TQ), F32), M((8, TQ), F32), M((8, TQ), F32),
            M((8, 128), F32), M((NH - 1, 8, 128), F32), M((16, 128), F32), M((NH - 1, 16, 128), F32),
            M((8, w, TQ), BF), M((8, w, TQ), BF), M((8, 8, TQ), F32), M((8, 8, TQ), F32),
            M((2, TQ, w), BF), M((NZ - 1, ar, w), BF), M((2, 8, TQ), F32), M((NZ - 1, 8, 128), F32), M((n, w), BF),
            D((10,)), D, D((NH - 1,)), D((NH - 1,)), D((NH - 1,)), D((NH - 1,)), D((6,)), D((6, NX * NZ)),
            D((8,)), D((8,)), D((8,)), D((8,)), D((NZ - 1,)), D((NZ - 1,)), D((NZ - 1,)), D((NZ - 1,)),
        ],
        compiler_params=pltpu.CompilerParams(collective_id=0, has_side_effects=True, vmem_limit_bytes=60 * 2**20),
        name="av_cross",
    )(video_q, video_k, video_v, audio_q, audio_k, audio_v, video_q_gain[None], audio_k_gain[None], audio_q_gain[None], video_k_gain[None])


def solution(mesh):
    return jax.shard_map(
        body,
        mesh=mesh,
        in_specs=(P("tok", "heads"),) * 6 + (P("heads"),) * 4,
        out_specs=(P("tok", "heads"), P("tok", "heads")),
        check_vma=False,
    )
```
